32 devices in a mesh: dp: 8 (over z, y), head: 4 (over x, core).
Axes of the slice: x: 2, y: 2, z: 4, core: 2. Of those that a mesh axis runs over, the one named last changes fastest.
Arguments:
- hidden: bfloat16 [1792, 16384], P('dp', 'head'), may hold values from -6 to 6
- norm_gain: float32 [16384], replicated, may hold values from 0.25 to 1.75
- query_weight: bfloat16 [16384, 2048], P('dp', 'head'), may hold values from -0.046875 to 0.046875
- kv_weight: bfloat16 [16384, 512], P(None, 'head'), may hold values from -0.046875 to 0.046875
- lengths: int32 [8, 2], replicated, may hold values from 28 to 112
- route_plan: int32 [8, 3], replicated, may hold values from 0 to 1
Outputs:
- attended: bfloat16 [1792, 2048], P('dp', 'head')
- fluctuation: float32 [2048], P('head')
- gram_matrix: float32 [8192, 8192], P('head', 'dp')
The draws below stay inside these ranges and needn't reach their ends.
All inputs are finite; a program needn't handle non-finite values.
Results may differ from the reference program's by a relative error of at most 0.0085.
Values may be sent and summed in bfloat16 or wider, within the bound.
No kernel may reach another device: no remote copies, remote signals or barrier semaphores. Data moves between devices by JAX's collectives and lax.ppermute only.
A program may use at most 128 MiB of HBM per device.

```python
import jax
import jax.numpy as jnp
from jax import lax

D = 16384
HD = 128
QH_DEV = 4
GW = 8192
SLOTS = 2
ROUNDS = 3
LMAX = 112
QHEADS = 16
KVH = 2
ROWS = 1792
N_DP = 8
N_HEAD = 4


def plant(values, rng, smallest, largest):
    extent = values.shape
    place = [jax.random.randint(jax.random.fold_in(rng, axis), (), 0, extent[axis]) for axis in range(len(extent))]
    values = values.at[tuple(place)].set(smallest)
    longest = extent.index(max(extent))
    place[longest] = (place[longest] + 1) % extent[longest]
    return values.at[tuple(place)].set(largest)


def block_levels(key, shape, cuts, smallest, top_value):
    loudness = 1.0
    for dim, blocks in cuts:
        draws = jax.random.uniform(jax.random.fold_in(jax.random.fold_in(key, 6), dim), (blocks,), jnp.float32, smallest / len(cuts), top_value / len(cuts))
        loudness = loudness * jnp.repeat(jnp.exp(draws), shape[dim] // blocks).reshape((-1,) + (1,) * (len(shape) - 1 - dim))
    return loudness


def gaussian(stream_key, extent, width, bound, pieces=(), kind=jnp.bfloat16):
    values = width * jax.random.normal(stream_key, extent, jnp.float32)
    if pieces:
        values = values * block_levels(stream_key, extent, pieces, -0.22, 0.18)
    return jnp.clip(values, -bound, bound).astype(kind)


def setup_inputs(seed: int = 0) -> dict:
    keys = jax.random.split(jax.random.key(seed), 7)
    hidden = gaussian(keys[0], (ROWS, D), 1.0, 6.0, ((0, 8), (1, 4)))
    norm_gain = jnp.clip(1.0 + 0.15 * jax.random.normal(keys[1], (D,), jnp.float32), 0.25, 1.75)
    query_weight = gaussian(keys[2], (D, QHEADS * HD), D ** -0.5, 0.046875, ((0, 8), (1, 4)))
    kv_weight = gaussian(keys[3], (D, KVH * 2 * HD), D ** -0.5, 0.046875, ((1, 4),))
    lengths = plant(jax.random.randint(keys[4], (N_DP, SLOTS), LMAX // 4, LMAX + 1), jax.random.fold_in(keys[4], 1), LMAX // 4, LMAX).astype(jnp.int32)
    route_plan = plant(jax.random.randint(keys[5], (N_DP, ROUNDS), 0, SLOTS), jax.random.fold_in(keys[5], 1), 0, SLOTS - 1).astype(jnp.int32)
    return dict(hidden=hidden, norm_gain=norm_gain, query_weight=query_weight, kv_weight=kv_weight, lengths=lengths, route_plan=route_plan)


rope_theta = 500000.0
norm_eps = 1e-05

def rotate(values_in, cosines, sines):
    middle = values_in.shape[-1] // 2
    front_half = values_in[..., :middle]
    back_half = values_in[..., middle:]
    return jnp.concatenate([front_half * cosines - back_half * sines, back_half * cosines + front_half * sines], axis=-1)

def reference(hidden, norm_gain, query_weight, kv_weight, lengths, route_plan):
    highest = lax.Precision.HIGHEST
    group_ids = jnp.arange(N_DP, dtype=jnp.int32)
    slot_ids = jnp.arange(SLOTS, dtype=jnp.int32)
    anchor = (group_ids[:, None] * SLOTS + slot_ids[None, :]).astype(jnp.int32)
    for round_bit in range(ROUNDS):
        leaving = route_plan[:, round_bit].astype(jnp.int32)
        handed = anchor[group_ids, leaving]
        partner = jnp.bitwise_xor(group_ids, 1 << round_bit).astype(jnp.int32)
        incoming = handed[partner]
        anchor = jnp.where(slot_ids[None, :] == leaving[:, None], incoming[:, None], anchor).astype(jnp.int32)
    batch = N_DP * SLOTS
    flat_anchor = anchor.reshape(batch).astype(jnp.int32)
    moved = hidden.reshape(batch, LMAX, D)[flat_anchor]
    moved_len = lengths.reshape(batch)[flat_anchor]
    positions = jnp.arange(LMAX, dtype=jnp.int32)
    row_count = batch * LMAX
    usable = (positions[None, :] < moved_len[:, None]).reshape(row_count)
    widened = moved.reshape(row_count, D).astype(jnp.float32)
    scaling = lax.rsqrt(lax.optimization_barrier(jnp.mean(widened * widened, axis=1, keepdims=True)) + norm_eps)
    normed = jnp.where(usable[:, None], widened * scaling * norm_gain[None, :], 0.0).astype(jnp.bfloat16)
    wide_normed = normed.astype(jnp.float32)
    query = jnp.dot(wide_normed, query_weight.astype(jnp.float32), precision=highest)
    head_total = QH_DEV * N_HEAD
    kv_total = N_HEAD // 2
    projected = jnp.dot(wide_normed, kv_weight.astype(jnp.float32), precision=highest).astype(jnp.bfloat16)
    projected = projected.reshape(row_count, kv_total, 2, HD)
    key_rows = projected[:, :, 0, :]
    value_rows = projected[:, :, 1, :]
    per_group = head_total // kv_total
    middle = HD // 2
    frequency = rope_theta ** (-(2.0 * jnp.arange(middle, dtype=jnp.float32) / HD))
    angles = jnp.tile(positions.astype(jnp.float32), batch)[:, None] * frequency[None, :]
    cosines = jnp.cos(angles)
    sines = jnp.sin(angles)
    rotated_query = rotate(query.reshape(row_count, head_total, HD), cosines[:, None, :], sines[:, None, :]).astype(jnp.bfloat16)
    rotated_keys = rotate(key_rows.astype(jnp.float32), cosines[:, None, :], sines[:, None, :]).astype(jnp.bfloat16)
    query_blocks = rotated_query.reshape(batch, LMAX, kv_total, per_group, HD).astype(jnp.float32)
    key_blocks = rotated_keys.reshape(batch, LMAX, kv_total, HD).astype(jnp.float32)
    value_blocks = value_rows.reshape(batch, LMAX, kv_total, HD).astype(jnp.float32)
    scores = jnp.einsum('blkgh,bmkh->bkglm', query_blocks, key_blocks, precision=highest) * HD ** (-0.5)
    key_usable = usable.reshape(batch, LMAX)
    allowed = (positions[None, :, None] >= positions[None, None, :]) & key_usable[:, None, :]
    exponent = jnp.where(allowed[:, None, None], jnp.exp(scores), 0.0)
    attn_probs = (exponent / lax.optimization_barrier(jnp.sum(exponent, axis=-1, keepdims=True))).astype(jnp.bfloat16)
    mixed_out = jnp.einsum('bkglm,bmkh->blkgh', attn_probs.astype(jnp.float32), value_blocks, precision=highest)
    attended = jnp.where(usable[:, None], mixed_out.reshape(row_count, head_total * HD), 0.0).astype(jnp.bfloat16)
    counted = jnp.sum(lengths).astype(jnp.float32)
    spread_in = attended.astype(jnp.float32)
    average = lax.optimization_barrier(jnp.sum(spread_in, axis=0)) / counted
    centered = jnp.where(usable[:, None], spread_in - average[None, :], 0.0)
    fluctuation = lax.optimization_barrier(jnp.sum(centered * centered, axis=0)) / (counted - 1.0)
    window = wide_normed[:, :GW]
    gram_matrix = jnp.dot(window.T, window, precision=highest) / counted
    return (attended, fluctuation, gram_matrix)
```

```python
import jax
import jax.numpy as jnp
from jax import lax
from jax.sharding import PartitionSpec as P

GW = 8192

rope_theta = 500000.0
norm_eps = 1e-05


def take(array, index, axis=0):
    return lax.dynamic_index_in_dim(array, index, axis, keepdims=False)


def partner_2(value, axis, stride):
    mask = 2**stride
    pairs = [(source, source ^ mask) for source in range(lax.axis_size(axis))]
    return lax.ppermute(value, axis, pairs)


def send(value, target):
    dp_count = lax.axis_size("dp")
    head_count = lax.axis_size("head")
    pairs = []
    for d in range(dp_count):
        for h in range(head_count):
            to = target(d, h)
            if to is not None:
                pairs.append((d * head_count + h, to[0] * head_count + to[1]))
    return lax.ppermute(value, ("dp", "head"), pairs)


def add_up(value, axis):
    stride = 0
    while 2**stride < lax.axis_size(axis):
        value = value + partner_2(value, axis, stride)
        stride += 1
    return value


def rotate(values_in, cosines, sines):
    middle = values_in.shape[-1] // 2
    front_half = values_in[..., :middle]
    back_half = values_in[..., middle:]
    return jnp.concatenate(
        [front_half * cosines - back_half * sines, back_half * cosines + front_half * sines],
        axis=-1,
    )


def factors(hidden, lengths, length_max):
    dp_count, slot_count = lengths.shape
    width = hidden.shape[1] * lax.axis_size("head")
    widened = hidden.astype(jnp.float32)
    local = jnp.sum(widened * widened, axis=1)
    table = jnp.zeros((dp_count, hidden.shape[0]), jnp.float32)
    table = lax.dynamic_update_slice_in_dim(table, local[None], lax.axis_index("dp"), 0)
    mean = add_up(add_up(table, "head"), "dp") / width
    positions = jnp.arange(length_max, dtype=jnp.int32)
    usable = positions[None, None, :] < lengths[:, :, None]
    return jnp.where(usable.reshape(mean.shape), lax.rsqrt(mean + norm_eps), 0.0)


def attend(query, keys, values, seq_lengths, length_max):
    slot_count = seq_lengths.shape[0]
    row_count, query_width = query.shape
    head_dim = keys.shape[1]
    heads_here = query_width // head_dim
    positions = jnp.arange(length_max, dtype=jnp.int32)
    usable = positions[None, :] < seq_lengths[:, None]
    middle = head_dim // 2
    frequency = rope_theta ** (-(2.0 * jnp.arange(middle, dtype=jnp.float32) / head_dim))
    angles = jnp.tile(positions.astype(jnp.float32), slot_count)[:, None] * frequency[None, :]
    cosines = jnp.cos(angles)
    sines = jnp.sin(angles)
    rotated_query = rotate(
        query.reshape(row_count, heads_here, head_dim), cosines[:, None, :], sines[:, None, :]
    ).astype(jnp.bfloat16)
    rotated_keys = rotate(keys.astype(jnp.float32), cosines, sines).astype(jnp.bfloat16)
    query_blocks = rotated_query.reshape(slot_count, length_max, heads_here, head_dim)
    key_blocks = rotated_keys.reshape(slot_count, length_max, head_dim)
    value_blocks = values.reshape(slot_count, length_max, head_dim)
    scores = jnp.einsum(
        "slqh,smh->sqlm", query_blocks, key_blocks, preferred_element_type=jnp.float32
    ) * head_dim ** (-0.5)
    allowed = (positions[None, :, None] >= positions[None, None, :]) & usable[:, None, :]
    exponent = jnp.where(allowed[:, None], jnp.exp(scores), 0.0)
    attn_probs = (exponent / jnp.sum(exponent, axis=-1, keepdims=True)).astype(jnp.bfloat16)
    mixed_out = jnp.einsum(
        "sqlm,smh->slqh", attn_probs, value_blocks, preferred_element_type=jnp.float32
    )
    return jnp.where(
        usable.reshape(row_count)[:, None], mixed_out.reshape(row_count, query_width), 0.0
    ).astype(jnp.bfloat16)


def trade(sequences, route_plan):
    group_index = lax.axis_index("dp")
    for round_bit in range(route_plan.shape[1]):
        leaving_here = take(route_plan[:, round_bit], group_index)
        arrived = partner_2(take(sequences, leaving_here), "dp", round_bit)
        sequences = lax.dynamic_update_index_in_dim(sequences, arrived, leaving_here, 0)
    return sequences


def project_any(hidden, norm_gain, query_weight, kv_weight, factor):
    whole = lax.all_gather(hidden, "head", axis=1, tiled=True)
    normed = (whole.astype(jnp.float32) * factor[:, None] * norm_gain[None, :]).astype(jnp.bfloat16)
    query = jnp.dot(
        normed,
        lax.all_gather(query_weight, "dp", axis=0, tiled=True),
        preferred_element_type=jnp.float32,
    )
    own_part = jnp.dot(normed, kv_weight, preferred_element_type=jnp.float32).astype(jnp.bfloat16)
    other_part = partner_2(own_part, "head", 0)
    leading = lax.axis_index("head") % 2 == 0
    keys = jnp.where(leading, own_part, other_part)
    values = jnp.where(leading, other_part, own_part)
    return query, keys, values, normed


def gram_any(normed, counted):
    head_count = lax.axis_size("head")
    columns = lax.all_to_all(normed[:, :GW], "dp", split_axis=1, concat_axis=0, tiled=True)
    span = GW // head_count
    own_rows = lax.dynamic_slice_in_dim(normed, lax.axis_index("head") * span, span, 1)
    rows = lax.all_gather(own_rows, "dp", axis=0, tiled=True)
    return (
        lax.dot_general(
            rows, columns, (((0,), (0,)), ((), ())), preferred_element_type=jnp.float32
        )
        / counted
    )


def project_planes(hidden, norm_gain, query_weight, kv_weight, slot_count):
    d, h = lax.axis_index("dp"), lax.axis_index("head")
    z, y, x, c = d // 2, d % 2, h // 2, h % 2
    w, p = z // 2, z % 2
    rows, cols = hidden.shape
    length_max = rows // slot_count
    sequences = hidden.reshape(slot_count, length_max, cols)

    def flip_x(value):
        return send(value, lambda d, h: (d, h ^ 2))

    def flip_core(value):
        return send(value, lambda d, h: (d, h ^ 1))

    keep = take(sequences, x)
    came = flip_x(take(sequences, 1 - x))
    other_rows = send(query_weight, lambda d, h: (d ^ 1, h))
    weight = jnp.where(
        y == 0,
        jnp.concatenate([query_weight, other_rows]),
        jnp.concatenate([other_rows, query_weight]),
    )
    kv_rows = lax.dynamic_slice_in_dim(kv_weight, z * cols, cols, 0)
    weight_twin = flip_core(weight)
    kv_twin = flip_core(kv_rows)
    gain = lax.dynamic_slice_in_dim(norm_gain, z * cols, cols, 0)

    def dot(tokens, matrix):
        return jnp.dot(tokens, matrix, preferred_element_type=jnp.float32).astype(jnp.bfloat16)

    total = None
    for e in range(2):
        block = jnp.where((w ^ e) == x, keep, came)

        def to_plane(d, h, e=e):
            z, y, x, c = d // 2, d % 2, h // 2, h % 2
            return 2 * (2 * ((z // 2) ^ e) + c) + y, 2 * x + z % 2

        mine = send(block, to_plane)
        tokens = jnp.concatenate([mine, flip_x(mine)])
        tokens = (tokens.astype(jnp.float32) * gain[None, :]).astype(jnp.bfloat16)
        own, twin = dot(tokens, weight), dot(tokens, weight_twin)
        kv_own, kv_other = dot(tokens, kv_rows), dot(tokens, kv_twin)
        keys = jnp.where(c == 0, kv_own, kv_other)
        values = jnp.where(c == 0, kv_other, kv_own)
        for f in range(2):
            chunk = jnp.concatenate(
                [jnp.where((p ^ f) == c, own, twin), keys, values], axis=1
            )

            def to_group(d, h, e=e, f=f):
                z, y, x, c = d // 2, d % 2, h // 2, h % 2
                return 2 * (2 * ((z // 2) ^ e) + c) + y, 2 * x + ((z % 2) ^ f)

            part = send(chunk, to_group).astype(jnp.float32)
            total = part if total is None else total + part
    return total


def gram_planes(hidden, norm_gain, factor, counted):
    dp_count = lax.axis_size("dp")
    z_count = dp_count // 2
    d, h = lax.axis_index("dp"), lax.axis_index("head")
    z, y = d // 2, d % 2
    span = hidden.shape[1] // 2
    first, second = hidden[:, :span], hidden[:, span:]
    near = send(
        jnp.where(h == 0, second, first), lambda d, h: (d, h + 1) if h < 2 else None
    )
    far = send(second, lambda d, h: (d, 3) if h == 1 else None)
    block = jnp.where(h == 0, first, jnp.where(h == 3, far, near))
    row_gain = lax.dynamic_slice_in_dim(norm_gain, h * span, span, 0)
    col_span = GW // dp_count
    col_gain = lax.dynamic_slice_in_dim(norm_gain, d * col_span, col_span, 0)

    def normed(values, scale, gain):
        return (values.astype(jnp.float32) * scale[:, None] * gain[None, :]).astype(jnp.bfloat16)

    row_parts, col_parts = [], []
    for step in range(z_count):
        if step:
            block = send(block, lambda d, h: ((d + 2) % dp_count, h))
        pair = jnp.concatenate([block, send(block, lambda d, h: (d ^ 1, h))])
        origin = 2 * ((z - step) % z_count) + y
        scale = jnp.concatenate([take(factor, origin), take(factor, origin ^ 1)])
        cut = lax.dynamic_slice_in_dim(pair, y * col_span, col_span, 1)
        across = send(cut, lambda d, h: (d, h ^ 2) if h == d // 2 else None)
        have = jnp.where(h == z, cut, across)
        twin = send(
            have, lambda d, h: (d, h ^ 1) if h in (d // 2, (d // 2) ^ 2) else None
        )
        columns = jnp.where((h == z) | (h == (z ^ 2)), have, twin)
        row_parts.append(normed(pair, scale, row_gain))
        col_parts.append(normed(columns, scale, col_gain))

    def dot(parts_a, parts_b):
        return lax.dot_general(
            jnp.concatenate(parts_a),
            jnp.concatenate(parts_b),
            (((0,), (0,)), ((), ())),
            preferred_element_type=jnp.float32,
        )

    early = dot(row_parts[:-1], col_parts[:-1])
    return (early + dot(row_parts[-1:], col_parts[-1:])) / counted


def on_device(hidden, norm_gain, query_weight, kv_weight, lengths, route_plan):
    dp_count = lax.axis_size("dp")
    head_count = lax.axis_size("head")
    group_index = lax.axis_index("dp")
    head_index = lax.axis_index("head")
    slot_count = lengths.shape[1]
    rows, cols = hidden.shape
    length_max = rows // slot_count
    head_dim = kv_weight.shape[1]
    query_width = query_weight.shape[1]
    counted = jnp.sum(lengths).astype(jnp.float32)
    factor = factors(hidden, lengths, length_max)
    own_factor = take(factor, group_index)
    own_lengths = take(lengths, group_index)
    planes = (
        head_count == 4
        and dp_count == 2 * head_count
        and slot_count == 2
        and GW == 2 * cols
        and cols == 2 * query_weight.shape[0]
    )
    if planes:
        swapped = head_index // 2 == 1
        total = project_planes(hidden, norm_gain, query_weight, kv_weight, slot_count)
        scale = own_factor.reshape(slot_count, length_max)
        scale = jnp.where(swapped, scale[::-1], scale).reshape(rows)
        seq_lengths = jnp.where(swapped, own_lengths[::-1], own_lengths)
        total = total * scale[:, None]
        query = total[:, :query_width]
        keys = total[:, query_width : query_width + head_dim].astype(jnp.bfloat16)
        values = total[:, query_width + head_dim :].astype(jnp.bfloat16)
        gram_matrix = gram_planes(hidden, norm_gain, factor, counted)
    else:
        query, keys, values, normed = project_any(
            hidden, norm_gain, query_weight, kv_weight, own_factor
        )
        seq_lengths = own_lengths
        gram_matrix = gram_any(normed, counted)
    attended = attend(query, keys, values, seq_lengths, length_max)
    spread_in = attended.astype(jnp.float32)
    summed, squared = add_up(
        jnp.stack([jnp.sum(spread_in, axis=0), jnp.sum(spread_in * spread_in, axis=0)]), "dp"
    )
    fluctuation = (squared - summed * summed / counted) / (counted - 1.0)
    slots = attended.reshape(slot_count, length_max, query_width)
    if planes:
        slots = jnp.where(swapped, slots[::-1], slots)
    attended = trade(slots, route_plan).reshape(rows, query_width)
    return (attended, fluctuation, gram_matrix)


def solution(mesh):
    return jax.shard_map(
        on_device,
        mesh=mesh,
        in_specs=(P("dp", "head"), P(), P("dp", "head"), P(None, "head"), P(), P()),
        out_specs=(P("dp", "head"), P("head"), P("head", "dp")),
        check_vma=False,
    )
```

```python
import jax
import jax.numpy as jnp
from jax import lax
from jax.sharding import PartitionSpec as P


GW = 8192

rope_theta = 500000.0
norm_eps = 1e-05


def take(array, index, axis=0):
    return lax.dynamic_index_in_dim(array, index, axis, keepdims=False)


def partner_2(value, axis, stride):
    mask = 2**stride
    pairs = [(source, source ^ mask) for source in range(lax.axis_size(axis))]
    return lax.ppermute(value, axis, pairs)


def send(value, target):
    dp_count = lax.axis_size("dp")
    head_count = lax.axis_size("head")
    pairs = []
    for d in range(dp_count):
        for h in range(head_count):
            to = target(d, h)
            if to is not None:
                pairs.append((d * head_count + h, to[0] * head_count + to[1]))
    return lax.ppermute(value, ("dp", "head"), pairs)


def add_up(value, axis):
    stride = 0
    while 2**stride < lax.axis_size(axis):
        value = value + partner_2(value, axis, stride)
        stride += 1
    return value


def rotate(values_in, cosines, sines):
    middle = values_in.shape[-1] // 2
    front_half = values_in[..., :middle]
    back_half = values_in[..., middle:]
    return jnp.concatenate(
        [front_half * cosines - back_half * sines, back_half * cosines + front_half * sines],
        axis=-1,
    )


def tie(value, after):
    return lax.optimization_barrier((value, after))[0]


def scale_by(values, factor, gain):
    return (values.astype(jnp.float32) * factor[:, None] * gain[None, :]).astype(jnp.bfloat16)


def norm_factor(local, width, seq_lengths, length_max):
    mean = add_up(local, "head") / width
    positions = jnp.arange(length_max, dtype=jnp.int32)
    usable = (positions[None, :] < seq_lengths[:, None]).reshape(mean.shape)
    return jnp.where(usable, lax.rsqrt(mean + norm_eps), 0.0)


def attend(query, keys, values, seq_lengths, length_max):
    slot_count = seq_lengths.shape[0]
    row_count, query_width = query.shape
    head_dim = keys.shape[1]
    heads_here = query_width // head_dim
    positions = jnp.arange(length_max, dtype=jnp.int32)
    usable = positions[None, :] < seq_lengths[:, None]
    middle = head_dim // 2
    frequency = rope_theta ** (-(2.0 * jnp.arange(middle, dtype=jnp.float32) / head_dim))
    angles = jnp.tile(positions.astype(jnp.float32), slot_count)[:, None] * frequency[None, :]
    cosines = jnp.cos(angles)
    sines = jnp.sin(angles)
    rotated_query = rotate(
        query.reshape(row_count, heads_here, head_dim), cosines[:, None, :], sines[:, None, :]
    ).astype(jnp.bfloat16)
    rotated_keys = rotate(keys.astype(jnp.float32), cosines, sines).astype(jnp.bfloat16)
    query_blocks = rotated_query.reshape(slot_count, length_max, heads_here, head_dim)
    key_blocks = rotated_keys.reshape(slot_count, length_max, head_dim)
    value_blocks = values.reshape(slot_count, length_max, head_dim)
    scores = jnp.einsum(
        "slqh,smh->sqlm", query_blocks, key_blocks, preferred_element_type=jnp.float32
    ) * head_dim ** (-0.5)
    allowed = (positions[None, :, None] >= positions[None, None, :]) & usable[:, None, :]
    exponent = jnp.where(allowed[:, None], jnp.exp(scores), 0.0)
    attn_probs = (exponent / jnp.sum(exponent, axis=-1, keepdims=True)).astype(jnp.bfloat16)
    mixed_out = jnp.einsum(
        "sqlm,smh->slqh", attn_probs, value_blocks, preferred_element_type=jnp.float32
    )
    return jnp.where(
        usable.reshape(row_count)[:, None], mixed_out.reshape(row_count, query_width), 0.0
    ).astype(jnp.bfloat16)


def trade(sequences, route_plan):
    group_index = lax.axis_index("dp")
    for round_bit in range(route_plan.shape[1]):
        leaving_here = take(route_plan[:, round_bit], group_index)
        arrived = partner_2(take(sequences, leaving_here), "dp", round_bit)
        sequences = lax.dynamic_update_index_in_dim(sequences, arrived, leaving_here, 0)
    return sequences


def keys_values(own_part):
    other_part = partner_2(own_part, "head", 0)
    leading = lax.axis_index("head") % 2 == 0
    keys = jnp.where(leading, own_part, other_part)
    values = jnp.where(leading, other_part, own_part)
    return keys, values


def project_any(hidden, norm_gain, query_weight, kv_weight, factor):
    whole = lax.all_gather(hidden, "head", axis=1, tiled=True)
    normed = scale_by(whole, factor, norm_gain)
    query = jnp.dot(
        normed,
        lax.all_gather(query_weight, "dp", axis=0, tiled=True),
        preferred_element_type=jnp.float32,
    )
    own_part = jnp.dot(normed, kv_weight, preferred_element_type=jnp.float32).astype(jnp.bfloat16)
    keys, values = keys_values(own_part)
    return query, keys, values, normed


def gram_any(normed, counted):
    head_count = lax.axis_size("head")
    columns = lax.all_to_all(normed[:, :GW], "dp", split_axis=1, concat_axis=0, tiled=True)
    span = GW // head_count
    own_rows = lax.dynamic_slice_in_dim(normed, lax.axis_index("head") * span, span, 1)
    rows = lax.all_gather(own_rows, "dp", axis=0, tiled=True)
    return (
        lax.dot_general(
            rows, columns, (((0,), (0,)), ((), ())), preferred_element_type=jnp.float32
        )
        / counted
    )


def flip_x(value):
    return send(value, lambda d, h: (d, h ^ 2))


def flip_core(value):
    return send(value, lambda d, h: (d, h ^ 1))


def flip_y(value):
    return send(value, lambda d, h: (d ^ 1, h))


def project_planes(keep, came, query_weight, other_rows, kv_weight):
    d, h = lax.axis_index("dp"), lax.axis_index("head")
    z, y, x, c = d // 2, d % 2, h // 2, h % 2
    w, p = z // 2, z % 2
    cols = keep.shape[1]
    weight = jnp.where(
        y == 0,
        jnp.concatenate([query_weight, other_rows]),
        jnp.concatenate([other_rows, query_weight]),
    )
    kv_rows = lax.dynamic_slice_in_dim(kv_weight, z * cols, cols, 0)
    matrix = jnp.concatenate([weight, kv_rows, flip_core(weight), flip_core(kv_rows)], axis=1)
    matrix = lax.optimization_barrier(matrix)
    half = matrix.shape[1] // 2
    total = None
    for e in range(2):

        def to_plane(d, h, e=e):
            z, y, x, c = d // 2, d % 2, h // 2, h % 2
            return 2 * (2 * ((z // 2) ^ e) + c) + y, 2 * x + z % 2

        def kept(d, h, e=e, to_plane=to_plane):
            return to_plane(d, h) if ((d // 4) ^ e) == h // 2 else None

        def passed(d, h, e=e, to_plane=to_plane):
            return to_plane(d, h) if ((d // 4) ^ e) != h // 2 else None

        mine = jnp.where(w == x, send(keep, kept), send(came, passed))
        tokens = jnp.concatenate([mine, flip_x(mine)])
        product = jnp.dot(tokens, matrix, preferred_element_type=jnp.float32)
        product = product.astype(jnp.bfloat16)
        for f in range(2):
            chunk = jnp.where((p ^ f) == c, product[:, :half], product[:, half:])

            def to_group(d, h, e=e, f=f):
                z, y, x, c = d // 2, d % 2, h // 2, h % 2
                return 2 * (2 * ((z // 2) ^ e) + c) + y, 2 * x + ((z % 2) ^ f)

            part = send(chunk, to_group).astype(jnp.float32)
            total = part if total is None else total + part
    return total


def arrival(up, down, z, step):
    last = len(up) - 1
    block = None
    for plane in range(last + 1):
        order = []
        for k in range(1, last + 1):
            if k <= plane:
                order.append(up[k])
            if k <= last - plane:
                order.append(down[k])
        mine = order[step - 1]
        block = mine if block is None else jnp.where(z == plane, mine, block)
    return block


def gram_planes(block, counted):
    dp_count = lax.axis_size("dp")
    last = dp_count // 2 - 1
    d, h = lax.axis_index("dp"), lax.axis_index("head")
    z, y = d // 2, d % 2
    col_span = GW // dp_count
    up, down = [block], [block]
    for step in range(1, last + 1):

        def rise(d, h, step=step):
            return (d + 2, h) if step - 1 <= d // 2 < last else None

        def sink(d, h, step=step):
            return (d - 2, h) if 0 < d // 2 <= last + 1 - step else None

        up.append(send(up[-1], rise))
        down.append(send(down[-1], sink))

    def dot(parts_a, parts_b):
        return lax.dot_general(
            jnp.concatenate(parts_a),
            jnp.concatenate(parts_b),
            (((0,), (0,)), ((), ())),
            preferred_element_type=jnp.float32,
        )

    row_parts, col_parts = [], []
    for step in range(last + 1):
        if step:
            block = arrival(up, down, tie(z, block), step)
        pair = jnp.concatenate([block, flip_y(block)])
        cut = lax.dynamic_slice_in_dim(pair, y * col_span, col_span, 1)
        if step == last:
            early = dot(row_parts, col_parts)
            early = lax.optimization_barrier(early)
        across = send(cut, lambda d, h: (d, h ^ 2) if h == d // 2 else None)
        have = jnp.where(h == z, cut, across)
        twin = send(have, lambda d, h: (d, h ^ 1) if h in (d // 2, (d // 2) ^ 2) else None)
        row_parts.append(pair)
        col_parts.append(jnp.where((h == z) | (h == (z ^ 2)), have, twin))
    return (dot(row_parts[-1:], col_parts[-1:]) + early) / counted


def planes(hidden, norm_gain, query_weight, kv_weight, own_lengths, length_max, counted):
    h = lax.axis_index("head")
    x = h // 2
    rows, cols = hidden.shape
    slot_count = rows // length_max
    span = cols // 2
    sequences = hidden.reshape(slot_count, length_max, cols)
    raw = flip_x(take(sequences, 1 - x))
    other_rows = flip_y(query_weight)
    widened = hidden.astype(jnp.float32)
    local = jnp.sum(widened * widened, axis=1)
    factor = norm_factor(local, cols * lax.axis_size("head"), own_lengths, length_max)
    slot_factor = take(factor.reshape(slot_count, length_max), x)
    keep = scale_by(
        take(sequences, x), slot_factor, lax.dynamic_slice_in_dim(norm_gain, h * cols, cols)
    )
    came = scale_by(
        raw, tie(slot_factor, keep), lax.dynamic_slice_in_dim(norm_gain, (h ^ 2) * cols, cols)
    )
    first, second = hidden[:, :span], hidden[:, span:]
    late = tie(h, raw)
    near = send(jnp.where(late == 0, second, first), lambda d, h: (d, h + 1) if h < 2 else None)
    far = send(jnp.where(late == 1, second, first), lambda d, h: (d, 3) if h == 1 else None)
    total = project_planes(keep, came, query_weight, other_rows, kv_weight)
    block = scale_by(
        jnp.where(h == 0, first, jnp.where(h == 3, far, near)),
        factor,
        lax.dynamic_slice_in_dim(norm_gain, h * span, span),
    )
    return total, gram_planes(block, counted)


def whole_step(hidden, norm_gain, query_weight, kv_weight, lengths, route_plan):
    dp_count = lax.axis_size("dp")
    head_count = lax.axis_size("head")
    group_index = lax.axis_index("dp")
    head_index = lax.axis_index("head")
    slot_count = lengths.shape[1]
    rows, cols = hidden.shape
    length_max = rows // slot_count
    query_width = query_weight.shape[1]
    counted = jnp.sum(lengths).astype(jnp.float32)
    own_lengths = take(lengths, group_index)
    by_planes = (
        plane_mesh(dp_count, head_count)
        and slot_count == 2
        and GW == 2 * cols
        and cols == 2 * query_weight.shape[0]
    )
    if by_planes:
        swapped = head_index // 2 == 1
        total, gram_matrix = planes(
            hidden, norm_gain, query_weight, kv_weight, own_lengths, length_max, counted
        )
        seq_lengths = jnp.where(swapped, own_lengths[::-1], own_lengths)
        query = total[:, :query_width]
        own_part = total[:, query_width:].astype(jnp.bfloat16)
        keys, values = keys_values(own_part)
    else:
        widened = hidden.astype(jnp.float32)
        factor = norm_factor(
            jnp.sum(widened * widened, axis=1), cols * head_count, own_lengths, length_max
        )
        query, keys, values, normed = project_any(
            hidden, norm_gain, query_weight, kv_weight, factor
        )
        seq_lengths = own_lengths
        gram_matrix = gram_any(normed, counted)
    attended = attend(query, keys, values, seq_lengths, length_max)
    spread_in = attended.astype(jnp.float32)
    summed, squared = add_up(
        jnp.stack([jnp.sum(spread_in, axis=0), jnp.sum(spread_in * spread_in, axis=0)]), "dp"
    )
    fluctuation = (squared - summed * summed / counted) / (counted - 1.0)
    slots = attended.reshape(slot_count, length_max, query_width)
    if by_planes:
        slots = jnp.where(swapped, slots[::-1], slots)
    attended = trade(slots, route_plan).reshape(rows, query_width)
    return (attended, fluctuation, gram_matrix)


def plane_mesh(dp_count, head_count):
    return head_count == 4 and dp_count == 2 * head_count


def solution(mesh):
    return jax.shard_map(
        whole_step,
        mesh=mesh,
        in_specs=(P("dp", "head"), P(), P("dp", "head"), P(None, "head"), P(), P()),
        out_specs=(P("dp", "head"), P("head"), P("head", "dp")),
        check_vma=False,
    )
```

```python
import jax
import jax.numpy as jnp
from jax import lax
from jax.sharding import PartitionSpec as P


GW = 8192

rope_theta = 500000.0
norm_eps = 1e-05


def take(array, index, axis=0):
    return lax.dynamic_index_in_dim(array, index, axis, keepdims=False)


def partner_2(value, axis, stride):
    mask = 2**stride
    pairs = [(source, source ^ mask) for source in range(lax.axis_size(axis))]
    return lax.ppermute(value, axis, pairs)


def send(value, target):
    dp_count = lax.axis_size("dp")
    head_count = lax.axis_size("head")
    pairs = []
    for d in range(dp_count):
        for h in range(head_count):
            to = target(d, h)
            if to is not None:
                pairs.append((d * head_count + h, to[0] * head_count + to[1]))
    return lax.ppermute(value, ("dp", "head"), pairs)


def add_up(value, axis):
    stride = 0
    while 2**stride < lax.axis_size(axis):
        value = value + partner_2(value, axis, stride)
        stride += 1
    return value


def rotate(values_in, cosines, sines):
    middle = values_in.shape[-1] // 2
    front_half = values_in[..., :middle]
    back_half = values_in[..., middle:]
    return jnp.concatenate(
        [front_half * cosines - back_half * sines, back_half * cosines + front_half * sines],
        axis=-1,
    )


def tie(value, after):
    return lax.optimization_barrier((value, after))[0]


def scale_by(values, factor, gain):
    return (values.astype(jnp.float32) * factor[:, None] * gain[None, :]).astype(jnp.bfloat16)


def norm_factor(local, width, seq_lengths, length_max):
    mean = add_up(local, "head") / width
    positions = jnp.arange(length_max, dtype=jnp.int32)
    usable = (positions[None, :] < seq_lengths[:, None]).reshape(mean.shape)
    return jnp.where(usable, lax.rsqrt(mean + norm_eps), 0.0)


def attend(query, keys, values, seq_lengths, length_max):
    slot_count = seq_lengths.shape[0]
    row_count, query_width = query.shape
    head_dim = keys.shape[1]
    heads_here = query_width // head_dim
    positions = jnp.arange(length_max, dtype=jnp.int32)
    usable = positions[None, :] < seq_lengths[:, None]
    middle = head_dim // 2
    frequency = rope_theta ** (-(2.0 * jnp.arange(middle, dtype=jnp.float32) / head_dim))
    angles = jnp.tile(positions.astype(jnp.float32), slot_count)[:, None] * frequency[None, :]
    cosines = jnp.cos(angles)
    sines = jnp.sin(angles)
    rotated_query = rotate(
        query.reshape(row_count, heads_here, head_dim), cosines[:, None, :], sines[:, None, :]
    ).astype(jnp.bfloat16)
    rotated_keys = rotate(keys.astype(jnp.float32), cosines, sines).astype(jnp.bfloat16)
    query_blocks = rotated_query.reshape(slot_count, length_max, heads_here, head_dim)
    key_blocks = rotated_keys.reshape(slot_count, length_max, head_dim)
    value_blocks = values.reshape(slot_count, length_max, head_dim)
    scores = jnp.einsum(
        "slqh,smh->sqlm", query_blocks, key_blocks, preferred_element_type=jnp.float32
    ) * head_dim ** (-0.5)
    allowed = (positions[None, :, None] >= positions[None, None, :]) & usable[:, None, :]
    exponent = jnp.where(allowed[:, None], jnp.exp(scores), 0.0)
    attn_probs = (exponent / jnp.sum(exponent, axis=-1, keepdims=True)).astype(jnp.bfloat16)
    mixed_out = jnp.einsum(
        "sqlm,smh->slqh", attn_probs, value_blocks, preferred_element_type=jnp.float32
    )
    return jnp.where(
        usable.reshape(row_count)[:, None], mixed_out.reshape(row_count, query_width), 0.0
    ).astype(jnp.bfloat16)


def trade(sequences, route_plan):
    group_index = lax.axis_index("dp")
    for round_bit in range(route_plan.shape[1]):
        leaving_here = take(route_plan[:, round_bit], group_index)
        arrived = partner_2(take(sequences, leaving_here), "dp", round_bit)
        sequences = lax.dynamic_update_index_in_dim(sequences, arrived, leaving_here, 0)
    return sequences


def keys_values(own_part):
    other_part = partner_2(own_part, "head", 0)
    leading = lax.axis_index("head") % 2 == 0
    keys = jnp.where(leading, own_part, other_part)
    values = jnp.where(leading, other_part, own_part)
    return keys, values


def project_any(hidden, norm_gain, query_weight, kv_weight, factor):
    whole = lax.all_gather(hidden, "head", axis=1, tiled=True)
    normed = scale_by(whole, factor, norm_gain)
    query = jnp.dot(
        normed,
        lax.all_gather(query_weight, "dp", axis=0, tiled=True),
        preferred_element_type=jnp.float32,
    )
    own_part = jnp.dot(normed, kv_weight, preferred_element_type=jnp.float32).astype(jnp.bfloat16)
    keys, values = keys_values(own_part)
    return query, keys, values, normed


def gram_any(normed, counted):
    head_count = lax.axis_size("head")
    columns = lax.all_to_all(normed[:, :GW], "dp", split_axis=1, concat_axis=0, tiled=True)
    span = GW // head_count
    own_rows = lax.dynamic_slice_in_dim(normed, lax.axis_index("head") * span, span, 1)
    rows = lax.all_gather(own_rows, "dp", axis=0, tiled=True)
    return (
        lax.dot_general(
            rows, columns, (((0,), (0,)), ((), ())), preferred_element_type=jnp.float32
        )
        / counted
    )


def flip_x(value):
    return send(value, lambda d, h: (d, h ^ 2))


def flip_core(value):
    return send(value, lambda d, h: (d, h ^ 1))


def flip_y(value):
    return send(value, lambda d, h: (d ^ 1, h))


def project_planes(keep, came, query_weight, other_rows, kv_weight):
    d, h = lax.axis_index("dp"), lax.axis_index("head")
    z, y, x, c = d // 2, d % 2, h // 2, h % 2
    w, p = z // 2, z % 2
    cols = keep.shape[1]
    weight = jnp.where(
        y == 0,
        jnp.concatenate([query_weight, other_rows]),
        jnp.concatenate([other_rows, query_weight]),
    )
    kv_rows = lax.dynamic_slice_in_dim(kv_weight, z * cols, cols, 0)
    matrix = jnp.concatenate([weight, kv_rows, flip_core(weight), flip_core(kv_rows)], axis=1)
    matrix = lax.optimization_barrier(matrix)
    half = matrix.shape[1] // 2
    total = None
    for e in range(2):

        def to_plane(d, h, e=e):
            z, y, x, c = d // 2, d % 2, h // 2, h % 2
            return 2 * (2 * ((z // 2) ^ e) + c) + y, 2 * x + z % 2

        def kept(d, h, e=e, to_plane=to_plane):
            moves = to_plane(d, h) != (d, h) and ((d // 4) ^ e) == h // 2
            return to_plane(d, h) if moves else None

        def passed(d, h, e=e, to_plane=to_plane):
            moves = to_plane(d, h) != (d, h) and ((d // 4) ^ e) != h // 2
            return to_plane(d, h) if moves else None

        sent_keep, sent_came = send(keep, kept), send(came, passed)
        if e == 0:
            sent_keep = jnp.where(p == c, keep, sent_keep)
            sent_came = jnp.where(p == c, came, sent_came)
        mine = jnp.where(w == x, sent_keep, sent_came)
        tokens = jnp.concatenate([mine, flip_x(mine)])
        product = jnp.dot(tokens, matrix, preferred_element_type=jnp.float32)
        product = product.astype(jnp.bfloat16)
        for f in range(2):
            chunk = jnp.where((p ^ f) == c, product[:, :half], product[:, half:])

            def to_group(d, h, e=e, f=f):
                z, y, x, c = d // 2, d % 2, h // 2, h % 2
                return 2 * (2 * ((z // 2) ^ e) + c) + y, 2 * x + ((z % 2) ^ f)

            def moved(d, h, to_group=to_group):
                return to_group(d, h) if to_group(d, h) != (d, h) else None

            part = send(chunk, moved)
            if e == 0 and f == 0:
                part = jnp.where(p == c, chunk, part)
            part = part.astype(jnp.float32)
            total = part if total is None else total + part
    return total


def arrival(up, down, z, step):
    last = len(up) - 1
    block = None
    for plane in range(last + 1):
        order = []
        for k in range(1, last + 1):
            if k <= plane:
                order.append(up[k])
            if k <= last - plane:
                order.append(down[k])
        mine = order[step - 1]
        block = mine if block is None else jnp.where(z == plane, mine, block)
    return block


def gram_planes(block, counted):
    dp_count = lax.axis_size("dp")
    last = dp_count // 2 - 1
    d, h = lax.axis_index("dp"), lax.axis_index("head")
    z, y = d // 2, d % 2
    col_span = GW // dp_count
    up, down = [block], [block]
    for step in range(1, last + 1):

        def rise(d, h, step=step):
            return (d + 2, h) if step - 1 <= d // 2 < last else None

        def sink(d, h, step=step):
            return (d - 2, h) if 0 < d // 2 <= last + 1 - step else None

        up.append(send(up[-1], rise))
        down.append(send(down[-1], sink))

    def dot(parts_a, parts_b):
        return lax.dot_general(
            jnp.concatenate(parts_a),
            jnp.concatenate(parts_b),
            (((0,), (0,)), ((), ())),
            preferred_element_type=jnp.float32,
        )

    row_parts, col_parts = [], []
    for step in range(last + 1):
        if step:
            block = arrival(up, down, tie(z, block), step)
        pair = jnp.concatenate([block, flip_y(block)])
        cut = lax.dynamic_slice_in_dim(pair, y * col_span, col_span, 1)
        if step == last - 1:
            early = dot(row_parts, col_parts)
            early = lax.optimization_barrier(early)
        across = send(cut, lambda d, h: (d, h ^ 2) if h == d // 2 else None)
        have = jnp.where(h == z, cut, across)
        twin = send(have, lambda d, h: (d, h ^ 1) if h in (d // 2, (d // 2) ^ 2) else None)
        row_parts.append(pair)
        col_parts.append(jnp.where((h == z) | (h == (z ^ 2)), have, twin))
    return (dot(row_parts[-2:], col_parts[-2:]) + early) / counted


def planes(hidden, norm_gain, query_weight, kv_weight, own_lengths, length_max, counted):
    h = lax.axis_index("head")
    x = h // 2
    rows, cols = hidden.shape
    slot_count = rows // length_max
    span = cols // 2
    sequences = hidden.reshape(slot_count, length_max, cols)
    first, second = hidden[:, :span], hidden[:, span:]
    near = send(jnp.where(h == 0, second, first), lambda d, h: (d, h + 1) if h < 2 else None)
    far = send(second, lambda d, h: (d, 3) if h == 1 else None)
    raw = flip_x(take(sequences, 1 - tie(x, (near, far))))
    other_rows = flip_y(query_weight)
    widened = hidden.astype(jnp.float32)
    local = jnp.sum(widened * widened, axis=1)
    factor = norm_factor(local, cols * lax.axis_size("head"), own_lengths, length_max)
    slot_factor = take(factor.reshape(slot_count, length_max), x)
    keep = scale_by(
        take(sequences, x), slot_factor, lax.dynamic_slice_in_dim(norm_gain, h * cols, cols)
    )
    came = scale_by(
        raw, tie(slot_factor, keep), lax.dynamic_slice_in_dim(norm_gain, (h ^ 2) * cols, cols)
    )
    total = project_planes(keep, came, query_weight, other_rows, kv_weight)
    block = scale_by(
        jnp.where(h == 0, first, jnp.where(h == 3, far, near)),
        factor,
        lax.dynamic_slice_in_dim(norm_gain, h * span, span),
    )
    return total, gram_planes(block, counted)


def whole_step(hidden, norm_gain, query_weight, kv_weight, lengths, route_plan):
    dp_count = lax.axis_size("dp")
    head_count = lax.axis_size("head")
    group_index = lax.axis_index("dp")
    head_index = lax.axis_index("head")
    slot_count = lengths.shape[1]
    rows, cols = hidden.shape
    length_max = rows // slot_count
    query_width = query_weight.shape[1]
    counted = jnp.sum(lengths).astype(jnp.float32)
    own_lengths = take(lengths, group_index)
    by_planes = (
        plane_mesh(dp_count, head_count)
        and slot_count == 2
        and GW == 2 * cols
        and cols == 2 * query_weight.shape[0]
    )
    if by_planes:
        swapped = head_index // 2 == 1
        total, gram_matrix = planes(
            hidden, norm_gain, query_weight, kv_weight, own_lengths, length_max, counted
        )
        seq_lengths = jnp.where(swapped, own_lengths[::-1], own_lengths)
        query = total[:, :query_width]
        own_part = total[:, query_width:].astype(jnp.bfloat16)
        keys, values = keys_values(own_part)
    else:
        widened = hidden.astype(jnp.float32)
        factor = norm_factor(
            jnp.sum(widened * widened, axis=1), cols * head_count, own_lengths, length_max
        )
        query, keys, values, normed = project_any(
            hidden, norm_gain, query_weight, kv_weight, factor
        )
        seq_lengths = own_lengths
        gram_matrix = gram_any(normed, counted)
    attended = attend(query, keys, values, seq_lengths, length_max)
    spread_in = attended.astype(jnp.float32)
    summed, squared = add_up(
        jnp.stack([jnp.sum(spread_in, axis=0), jnp.sum(spread_in * spread_in, axis=0)]), "dp"
    )
    fluctuation = (squared - summed * summed / counted) / (counted - 1.0)
    slots = attended.reshape(slot_count, length_max, query_width)
    if by_planes:
        slots = jnp.where(swapped, slots[::-1], slots)
    attended = trade(slots, route_plan).reshape(rows, query_width)
    return (attended, fluctuation, gram_matrix)


def plane_mesh(dp_count, head_count):
    return head_count == 4 and dp_count == 2 * head_count


def solution(mesh):
    return jax.shard_map(
        whole_step,
        mesh=mesh,
        in_specs=(P("dp", "head"), P(), P("dp", "head"), P(None, "head"), P(), P()),
        out_specs=(P("dp", "head"), P("head"), P("head", "dp")),
        check_vma=False,
    )
```
